32 devices in a mesh: dp: 8 (over y, x, core), mp: 4 (over z).
Axes of the slice: x: 2, y: 2, z: 4, core: 2. Of those that a mesh axis runs over, the one named last changes fastest.
Arguments:
- mel_audio: bfloat16 [32, 80, 2048], P('dp'), may hold values from -6 to 6
- start_noise: bfloat16 [32, 80, 1024], P('dp'), may hold values from -6 to 6
- span_start: int32 [32], replicated, may hold values from 0 to 2047, as said below
- span_length: int32 [32], replicated, may hold values from 1 to 1024, as said below
- block_route: int32 [128], replicated, may hold values from -1 to 47, as said below
- w_input: bfloat16 [160, 1024], replicated, may hold values from -0.5 to 0.5
- attn_gain: float32 [1024], replicated, may hold values from 0.1 to 1.9
- w_qkv: bfloat16 [1024, 3, 1024], P(None, None, 'mp'), may hold values from -4 to 4, as said below
- w_out: bfloat16 [1024, 1024], P('mp'), may hold values from -0.1875 to 0.1875
- final_gain: float32 [1024], replicated, may hold values from 0.1 to 1.9
- w_mel: bfloat16 [80, 1024], replicated, may hold values from -0.1875 to 0.1875
Outputs:
- infilled: float32 [32, 80, 1024], P('dp')
- worker_velocity: float32 [48, 80, 256], P('dp')
The draws below stay inside these ranges and needn't reach their ends.
Inputs may be any that keep to these rules, and one draw needn't show every extreme that they name: Each span lies inside its utterance: span_start[u] + span_length[u] <= 2048. `span_length`: the spans cover 48 blocks of 256 frames in all (the last block of a span may be partly filled). `block_route`: live block slots name worker slots w * 6 + j of worker w, each worker slot exactly once; empty slots hold -1. No worker receives more than 2 blocks from the utterances of one dp index (utterances u with the same u // 4), and some worker receives exactly 2 from one. `w_qkv`: Query, key and value projections in that order along the middle dimension.
All inputs are finite; a program needn't handle non-finite values.
Results may differ from the reference program's by a relative error of at most 0.025.
Values may be sent and summed in bfloat16 or wider, within the bound.
A program may use at most 128 MiB of HBM per device.

```python
import math
import jax
import jax.numpy as jnp
from jax import lax

D = 1024
HEADS = 16
MEL = 80
HEAD_DIM = 64
BLOCK = 256
CTX = 128
BLK_UTT = 4
UTT_DEV = 4
WORK_DEV = 6
EULER = 2
FRAMES = 2048
WIN = 512
SPAN_MAX = 1024
UTTS = 32
SLOTS_ALL = 128
WORK_ALL = 48
N_MP = 4


def span_plan(key):
    split_keys = jax.random.split(jax.random.fold_in(key, 4111), 5)
    spare_blocks = BLK_UTT - 1
    cell_count = UTTS * spare_blocks
    extra_blocks = WORK_ALL - UTTS
    worker_count = WORK_ALL // WORK_DEV
    shuffled = jax.random.permutation(split_keys[0], cell_count)
    cell_rank = jnp.argsort(shuffled, stable=True).astype(jnp.int32)
    chosen = jax.random.randint(split_keys[1], (), 0, UTTS)
    cell_ids = jnp.arange(cell_count, dtype=jnp.int32)
    forced = cell_ids // spare_blocks // UTT_DEV == chosen // UTT_DEV
    cell_score = jnp.where(forced, cell_ids - cell_count, cell_rank)
    placing = jnp.argsort(jnp.argsort(cell_score, stable=True), stable=True)
    taken_mask = (placing < extra_blocks).astype(jnp.int32)
    counts = 1 + jnp.sum(taken_mask.reshape(UTTS, spare_blocks), axis=1)
    remainder = jax.random.randint(split_keys[2], (UTTS,), 1, BLOCK + 1)
    remainder = jnp.where(jnp.arange(UTTS) == chosen, BLOCK, remainder)
    length = (counts - 1) * BLOCK + remainder
    first_frame = jax.random.randint(split_keys[3], (UTTS,), 0, FRAMES - length + 1)
    live_slots = (jnp.arange(BLK_UTT)[None, :] < counts[:, None]).reshape(-1).astype(jnp.int32)
    live_order = jnp.cumsum(live_slots) - live_slots
    workers = jax.random.permutation(split_keys[4], worker_count)
    worker = workers[live_order % worker_count]
    route_table = jnp.where(live_slots > 0, worker * WORK_DEV + live_order // worker_count, -1)
    return (first_frame.astype(jnp.int32), length.astype(jnp.int32), route_table.astype(jnp.int32))


def draw_span_start(key, part):
    return span_plan(key)[0]


def draw_span_length(key, part):
    return span_plan(key)[1]


def draw_block_route(key, part):
    return span_plan(key)[2]


def draw_w_qkv(key, part):
    split_keys = jax.random.split(jax.random.fold_in(key, 977), 1)
    scale = 1.0 / math.sqrt(D)
    drawn = jnp.clip(jax.random.normal(split_keys[0], (D, 3, D)), -6.0, 6.0) * scale
    return drawn.astype(jnp.bfloat16)


def level_of(own_key, shape, pieces, smallest, largest):
    def one(dim, shards_of):
        steps = jax.random.uniform(jax.random.fold_in(jax.random.fold_in(own_key, 6), dim), (shards_of,), jnp.float32, smallest / len(pieces), largest / len(pieces))
        return jnp.repeat(jnp.exp(steps), shape[dim] // shards_of).reshape((-1,) + (1,) * (len(shape) - dim - 1))

    loudness = one(*pieces[0])
    for cut in pieces[1:]:
        loudness = loudness * one(*cut)
    return loudness


def scatter_about(key, extent, scale, limit, cuts=(), held_as=jnp.bfloat16):
    level = level_of(key, extent, cuts, -0.22, 0.18) if cuts else 1.0
    array = jax.random.normal(key, extent, jnp.float32) * scale * level
    return jnp.minimum(jnp.maximum(array, -limit), limit).astype(held_as)


def setup_inputs(seed: int = 0) -> dict:
    arg_keys = jax.random.split(jax.random.key(seed), 12)
    return {
        "mel_audio": scatter_about(arg_keys[0], (UTTS, MEL, FRAMES), 1.0, 6.0, ((0, 8),)),
        "start_noise": scatter_about(arg_keys[1], (UTTS, MEL, SPAN_MAX), 1.0, 6.0, ((0, 8),)),
        "span_start": draw_span_start(jax.random.fold_in(arg_keys[11], 71), 0),
        "span_length": draw_span_length(jax.random.fold_in(arg_keys[11], 71), 0),
        "block_route": draw_block_route(jax.random.fold_in(arg_keys[11], 71), 0),
        "w_input": scatter_about(arg_keys[5], (2 * MEL, D), (2 * MEL) ** -0.5, 0.5),
        "attn_gain": jnp.clip(1.0 + 0.18 * jax.random.normal(arg_keys[6], (D,), jnp.float32), 0.1, 1.9),
        "w_qkv": draw_w_qkv(jax.random.fold_in(arg_keys[11], 71), 0),
        "w_out": scatter_about(arg_keys[8], (D, D), D ** -0.5, 0.1875, ((0, 4),)),
        "final_gain": jnp.clip(1.0 + 0.18 * jax.random.normal(arg_keys[9], (D,), jnp.float32), 0.1, 1.9),
        "w_mel": scatter_about(arg_keys[10], (MEL, D), D ** -0.5, 0.1875),
    }


flow_steps = 32.0
norm_eps = 1e-05

def time_embed(t_value, feature_width):
    half_width = feature_width // 2
    freqs = jnp.exp(-math.log(10000.0) * jnp.arange(half_width, dtype=jnp.float32) / half_width)
    angles = 1000.0 * t_value * freqs
    return jnp.concatenate([jnp.sin(angles), jnp.cos(angles)])

def layer_norm(hidden, norm_gain):
    mean_value = lax.optimization_barrier(jnp.mean(hidden, axis=-1, keepdims=True))
    centred = hidden - mean_value
    variance = lax.optimization_barrier(jnp.mean(centred * centred, axis=-1, keepdims=True))
    return centred * lax.rsqrt(variance + norm_eps) * norm_gain.astype(jnp.float32)

def velocity(window, window_begin, own_count, t_value, w_input, attn_gain, w_qkv, w_out, final_gain, w_mel):
    hidden = jnp.dot(window.T, w_input, preferred_element_type=jnp.float32)
    hidden = hidden + time_embed(t_value, D)[None, :]
    normed = layer_norm(hidden, attn_gain).astype(jnp.bfloat16)
    queries = jnp.dot(normed[CTX:CTX + BLOCK], w_qkv[:, 0, :], preferred_element_type=jnp.float32).astype(jnp.bfloat16)
    key_rows = jnp.dot(normed, w_qkv[:, 1, :], preferred_element_type=jnp.float32).astype(jnp.bfloat16)
    value_rows = jnp.dot(normed, w_qkv[:, 2, :], preferred_element_type=jnp.float32).astype(jnp.bfloat16)
    query_heads = queries.astype(jnp.float32).reshape(BLOCK, HEADS, HEAD_DIM)
    key_heads = key_rows.astype(jnp.float32).reshape(WIN, HEADS, HEAD_DIM)
    value_heads = value_rows.astype(jnp.float32).reshape(WIN, HEADS, HEAD_DIM)
    scores = jnp.einsum('qhd,khd->hqk', query_heads, key_heads) * (1.0 / math.sqrt(HEAD_DIM))
    position = window_begin - CTX + jnp.arange(WIN, dtype=jnp.int32)
    usable = (position >= 0) & (position < FRAMES)
    scores = jnp.where(usable[None, None, :], scores, -1e+30)
    attn_weights = jax.nn.softmax(scores, axis=-1).astype(jnp.bfloat16)
    head_outputs = jnp.einsum('hqk,khd->qhd', attn_weights.astype(jnp.float32), value_heads)
    head_outputs = head_outputs.astype(jnp.bfloat16).reshape(BLOCK, D)
    group_width = D // N_MP
    attended = jnp.zeros((BLOCK, D), jnp.float32)
    for mp_part in range(N_MP):
        lower = mp_part * group_width
        term = jnp.dot(head_outputs[:, lower:lower + group_width], w_out[lower:lower + group_width], preferred_element_type=jnp.float32)
        attended = attended + term.astype(jnp.bfloat16).astype(jnp.float32)
    final = layer_norm(hidden[CTX:CTX + BLOCK] + attended, final_gain).astype(jnp.bfloat16)
    result = jnp.dot(w_mel, final.T, preferred_element_type=jnp.float32)
    live_mask = jnp.arange(BLOCK, dtype=jnp.int32) < own_count
    return jnp.where(live_mask[None, :], result, 0.0)

def reference(mel_audio, start_noise, span_start, span_length, block_route, w_input, attn_gain, w_qkv, w_out, final_gain, w_mel):
    slot_ids = jnp.arange(WORK_ALL, dtype=jnp.int32)
    every_slot = jnp.arange(SLOTS_ALL, dtype=jnp.int32)
    matches = block_route[None, :] == slot_ids[:, None]
    blocks = lax.optimization_barrier(jnp.sum(jnp.where(matches, every_slot[None, :], 0), axis=1)).astype(jnp.int32)
    padded = jnp.pad(mel_audio, ((0, 0), (0, 0), (CTX, SPAN_MAX + CTX)))
    zero_index = jnp.zeros((), jnp.int32)

    def solve_block(block_index):
        utterance = (block_index // BLK_UTT).astype(jnp.int32)
        block_order = (block_index % BLK_UTT).astype(jnp.int32)
        first_frame = span_start[utterance]
        length = span_length[utterance]
        window_begin = (first_frame + BLOCK * block_order).astype(jnp.int32)
        audio_rows = lax.dynamic_slice(padded, (utterance, zero_index, window_begin), (1, MEL, WIN))[0]
        position = window_begin - CTX + jnp.arange(WIN, dtype=jnp.int32)
        in_span = (position >= first_frame) & (position < first_frame + length)
        context = jnp.where(in_span[None, :], jnp.zeros((), jnp.bfloat16), audio_rows)
        own_count = jnp.minimum(BLOCK, length - BLOCK * block_order)
        live_mask = jnp.arange(BLOCK, dtype=jnp.int32) < own_count
        frames_state = lax.dynamic_slice(start_noise, (utterance, zero_index, (BLOCK * block_order).astype(jnp.int32)), (1, MEL, BLOCK))[0].astype(jnp.float32)
        side_zeros = jnp.zeros((MEL, CTX), jnp.bfloat16)
        result = jnp.zeros((MEL, BLOCK), jnp.float32)
        total = jnp.zeros((MEL, BLOCK), jnp.float32)
        for euler_step in range(EULER):
            state_rows = jnp.where(live_mask[None, :], frames_state, 0.0).astype(jnp.bfloat16)
            state_window = jnp.concatenate([side_zeros, state_rows, side_zeros], axis=1)
            window = jnp.concatenate([context, state_window], axis=0)
            result = velocity(window, window_begin, own_count, euler_step / flow_steps, w_input, attn_gain, w_qkv, w_out, final_gain, w_mel)
            frames_state = frames_state + result * (1.0 / flow_steps)
            total = total + result
        return (result, jnp.where(live_mask[None, :], total, 0.0))
    worker_velocity, finals = lax.map(solve_block, blocks)
    slotted = jnp.zeros((SLOTS_ALL, MEL, BLOCK), jnp.float32).at[blocks].set(finals)
    infilled = slotted.reshape(UTTS, BLK_UTT, MEL, BLOCK).transpose(0, 2, 1, 3).reshape(UTTS, MEL, SPAN_MAX)
    return (infilled, worker_velocity)
```

```python
import functools
import math

import jax
import jax.numpy as jnp
import numpy as np
from jax import lax
from jax.experimental import pallas as pl
from jax.experimental.pallas import tpu as pltpu
from jax.sharding import PartitionSpec as P

MEL = 80
HEAD_DIM = 64
BLOCK = 256
CTX = 128
BLK_UTT = 4
UTT_DEV = 4
WORK_DEV = 6
EULER = 2
FRAMES = 2048
WIN = 512
SPAN_MAX = 1024
SLOT_DEV = 16
LANES = 128
PIECES = 8

flow_steps = 32.0
norm_eps = 1e-05
MESH = pl.DeviceIdType.MESH
VMEM_LIMIT = 60 * 1024 * 1024
F32 = jnp.float32
BF16 = jnp.bfloat16


def time_table(width):
    half = width // 2
    freqs = np.exp(-math.log(10000.0) * np.arange(half, dtype=np.float64) / half)
    rows = []
    for step in range(EULER):
        angles = 1000.0 * (step / flow_steps) * freqs
        rows.append(np.concatenate([np.sin(angles), np.cos(angles)]))
    return np.stack(rows).astype(np.float32)


def flip(index, bit):
    return index + bit * (1 - 2 * ((index // bit) % 2))


def pick(index, values):
    out = jnp.int32(values[-1])
    for i in range(len(values) - 1):
        out = jnp.where(index == i, jnp.int32(values[i]), out)
    return out


def shard_order(count):
    return [
        sorted((s for s in range(count) if s != m), key=lambda s: (abs(s - m), s))
        for m in range(count)
    ]


def remote(src, dst, send_sem, recv_sem, device):
    return pltpu.make_async_remote_copy(
        src_ref=src,
        dst_ref=dst,
        send_sem=send_sem,
        recv_sem=recv_sem,
        device_id=device,
        device_id_type=MESH,
    )


def enter(n_dp, n_mp, dp, mp):
    barrier = pltpu.get_barrier_semaphore()
    for t in range(1, n_dp):
        pl.semaphore_signal(
            barrier, inc=1, device_id={"dp": (dp + t) % n_dp}, device_id_type=MESH
        )
    for t in range(1, n_mp):
        pl.semaphore_signal(
            barrier, inc=1, device_id={"mp": (mp + t) % n_mp}, device_id_type=MESH
        )
    pl.semaphore_wait(barrier, n_dp + n_mp - 2)


def blocks_between(blocks_ref, worker, owner, capacity):
    blocks = [jnp.int32(-1)] * capacity
    slots = [jnp.int32(-1)] * capacity
    seen = jnp.int32(0)
    for j in range(WORK_DEV):
        block = blocks_ref[worker * WORK_DEV + j]
        mine = (block // SLOT_DEV) == owner
        for r in range(capacity):
            here = mine & (seen == r)
            blocks[r] = jnp.where(here, block, blocks[r])
            slots[r] = jnp.where(here, j, slots[r])
        seen = seen + mine.astype(jnp.int32)
    return blocks, slots


def choose(wanted, ids, parts):
    out = jnp.zeros_like(parts[0])
    for n, part in zip(ids, parts):
        out = jnp.where(wanted == n, part, out)
    return out


def pair_slots(mp):
    return 3 * (mp // 2) + 2 * (mp % 2), 3 * (mp // 2) + 1


class WeightGather:
    def __init__(self, n_mp, dp, mp, w_all, sems):
        self.n_mp, self.dp, self.mp, self.w_all = n_mp, dp, mp, w_all
        (self.zs, self.zf, self.zr, self.xs, self.xr, self.ys, self.yr, self.cs, self.cr) = sems
        self.rows = w_all.shape[2] // PIECES
        self.half = self.rows // 2
        base = dp - dp % PIECES
        part = dp % PIECES
        self.part = part
        self.x_peer = {"dp": base + flip(part, 2)}
        self.y_peer = {"dp": base + flip(part, 4)}
        self.c_peer = {"dp": base + flip(part, 1)}
        self.order = shard_order(n_mp)

    def view(self, shard, part, half):
        start = pl.multiple_of(part * self.rows + half * self.half, self.half)
        return self.w_all.at[shard, :, pl.ds(start, self.half), :]

    def shard(self, i):
        return pick(self.mp, [self.order[m][i] for m in range(self.n_mp)])

    def z_copy(self, shard, half, step, send_sem):
        view = self.view(shard, self.part, half)
        return remote(view, view, send_sem, self.zr.at[shard, half], {"mp": self.mp + step})

    def z_arrival(self, shard, half):
        view = self.view(shard, self.part, half)
        sem = self.zf.at[shard, half]
        return remote(view, view, sem, self.zr.at[shard, half], {"mp": (self.mp + 1) % self.n_mp})

    def send_own(self):
        @pl.when(self.mp + 1 < self.n_mp)
        def _():
            for half in range(2):
                self.z_copy(self.mp, half, 1, self.zs.at[0, half]).start()

        @pl.when(self.mp > 0)
        def _():
            for half in range(2):
                self.z_copy(self.mp, half, -1, self.zs.at[1, half]).start()

    def relay(self, shard, half, act):
        @pl.when((shard < self.mp) & (self.mp + 1 < self.n_mp))
        def _():
            act(self.z_copy(shard, half, 1, self.zf.at[shard, half]))

        @pl.when((shard > self.mp) & (self.mp > 0))
        def _():
            act(self.z_copy(shard, half, -1, self.zf.at[shard, half]))

    def x_copy(self, shard, part, half, kind):
        view = self.view(shard, part, half)
        return remote(
            view, view, self.xs.at[shard, kind], self.xr.at[shard, kind], self.x_peer
        )

    def y_copy(self, shard, part, half, kind):
        view = self.view(shard, part, half)
        return remote(
            view, view, self.ys.at[shard, kind], self.yr.at[shard, kind], self.y_peer
        )

    def c_copy(self, shard, part, half, kind):
        view = self.view(shard, part, half)
        return remote(
            view, view, self.cs.at[shard, kind], self.cr.at[shard, kind], self.c_peer
        )

    def own_piece(self, i):
        shard = self.shard(i)
        for half in range(2):
            self.z_arrival(shard, half).wait_recv()
            self.relay(shard, half, lambda copy: copy.start())
            self.x_copy(shard, self.part, half, half).start()
            self.y_copy(shard, self.part, half, half).start()
            self.c_copy(shard, self.part, half, half).start()

    def near_pieces(self, i):
        shard = self.shard(i)
        from_x, from_y = flip(self.part, 2), flip(self.part, 4)
        self.x_copy(shard, from_x, 0, 0).wait_recv()
        self.y_copy(shard, from_x, 0, 2).start()
        self.c_copy(shard, from_x, 0, 2).start()
        self.y_copy(shard, from_y, 0, 0).wait_recv()
        self.c_copy(shard, from_y, 0, 4).start()
        self.y_copy(shard, from_y, 1, 1).wait_recv()
        self.x_copy(shard, from_y, 1, 2).start()
        self.c_copy(shard, from_y, 1, 5).start()
        self.x_copy(shard, from_x, 1, 1).wait_recv()
        self.c_copy(shard, from_x, 1, 3).start()

    def far_pieces(self, i):
        shard = self.shard(i)
        far = flip(flip(self.part, 2), 4)
        self.y_copy(shard, far, 0, 2).wait_recv()
        self.c_copy(shard, far, 0, 6).start()
        self.x_copy(shard, far, 1, 2).wait_recv()
        self.c_copy(shard, far, 1, 7).start()

    def arrived(self, i):
        shard = self.shard(i)
        other = flip(self.part, 1)
        parts = [other, flip(other, 2), flip(other, 4), flip(flip(other, 2), 4)]
        for n, part in enumerate(parts):
            for half in range(2):
                self.c_copy(shard, part, half, 2 * n + half).wait_recv()

    def drain(self):
        for half in range(2):

            @pl.when(self.mp + 1 < self.n_mp)
            def _():
                self.z_copy(self.mp, half, 1, self.zs.at[0, half]).wait_send()

            @pl.when(self.mp > 0)
            def _():
                self.z_copy(self.mp, half, -1, self.zs.at[1, half]).wait_send()

        for i in range(self.n_mp - 1):
            shard = self.shard(i)
            for half in range(2):
                self.relay(shard, half, lambda copy: copy.wait_send())
            for kind in range(3):
                self.x_copy(shard, self.part, 0, kind).wait_send()
                self.y_copy(shard, self.part, 0, kind).wait_send()
            for kind in range(8):
                self.c_copy(shard, self.part, 0, kind).wait_send()


def gather_sems(n_mp):
    dma = pltpu.SemaphoreType.DMA
    return [
        dma((2, 2)),
        dma((n_mp, 2)),
        dma((n_mp, 2)),
        dma((n_mp, 3)),
        dma((n_mp, 3)),
        dma((n_mp, 3)),
        dma((n_mp, 3)),
        dma((n_mp, 8)),
        dma((n_mp, 8)),
    ]


def pack_windows(mel_ref, noise_ref, start_ref, length_ref, dp, mp, local):
    start = start_ref[dp * UTT_DEV + local]
    length = length_ref[dp * UTT_DEV + local]
    first = start - CTX + LANES * mp
    chunk = (first + LANES) // LANES
    offset = first + LANES - chunk * LANES
    count = 2 * BLK_UTT
    zero = jnp.zeros((MEL, LANES), BF16)
    chunks = [zero]
    for n in range(FRAMES // LANES):
        chunks.append(mel_ref[local, :, n * LANES : (n + 1) * LANES])
    bit = 1
    while 2 * bit <= len(chunks):
        bit *= 2
    while bit:
        moved = (chunk // bit) % 2 == 1
        keep = min(len(chunks), count + bit - 1)
        padded = chunks + [zero] * (keep + bit - len(chunks))
        chunks = [jnp.where(moved, padded[n + bit], padded[n]) for n in range(keep)]
        bit //= 2
    row = lax.broadcasted_iota(jnp.int32, (2 * LANES, LANES), 0)
    to = lax.broadcasted_iota(jnp.int32, (2 * LANES, LANES), 1)
    shift = jnp.where(row == to + offset, 1.0, 0.0).astype(BF16)
    both = jnp.concatenate(
        [jnp.concatenate(chunks[2 * k : 2 * k + 2], axis=1) for k in range(BLK_UTT)], axis=0
    )
    shifted = lax.dot_general(
        both, shift, (((1,), (0,)), ((), ())), preferred_element_type=F32
    )
    lane = lax.broadcasted_iota(jnp.int32, (MEL, LANES), 1)
    parts = []
    for k in range(BLK_UTT):
        frame = first + BLOCK * k + lane
        context = (frame >= 0) & (frame < FRAMES) & ((frame < start) | (frame >= start + length))
        own = jnp.minimum(BLOCK, length - BLOCK * k)
        place = LANES * (mp - 1) + lane
        state = (place >= 0) & (place < own)
        noise = jnp.where(
            mp == 2,
            noise_ref[local, :, BLOCK * k + LANES : BLOCK * k + 2 * LANES].astype(F32),
            noise_ref[local, :, BLOCK * k : BLOCK * k + LANES].astype(F32),
        )
        held = jnp.where(context, shifted[k * MEL : (k + 1) * MEL], 0.0)
        parts.append(jnp.where(state, noise, held).astype(BF16))
    return parts


def inbound_kernel(
    n_dp,
    n_mp,
    capacity,
    blocks_ref,
    start_ref,
    length_ref,
    mel_ref,
    noise_ref,
    w_qkv_ref,
    w_out_ref,
    w_all,
    win,
    packed,
    landed,
    sorted_parts,
    spread,
    load_sem,
    d_send,
    d_recv,
    m_send,
    m_recv,
    *w_sems,
):
    dp, mp = lax.axis_index("dp"), lax.axis_index("mp")
    width = w_all.shape[3]
    loads = [pltpu.make_async_copy(w_qkv_ref, w_all.at[mp, 0:3], load_sem.at[0])]
    for n in range(n_mp):
        loads.append(
            pltpu.make_async_copy(
                w_out_ref.at[:, n * width : (n + 1) * width],
                w_all.at[mp, 3, n * width : (n + 1) * width, :],
                load_sem.at[1 + n],
            )
        )
    for load in loads:
        load.start()
    enter(n_dp, n_mp, dp, mp)
    for load in loads:
        load.wait()
    gather = WeightGather(n_mp, dp, mp, w_all, w_sems)
    gather.send_own()

    def to_worker(t):
        worker = (dp + t) % n_dp
        return worker, remote(
            packed.at[worker], landed.at[dp], d_send.at[t], d_recv.at[t], {"dp": worker}
        )

    parts = []
    for local in range(UTT_DEV):
        parts += pack_windows(mel_ref, noise_ref, start_ref, length_ref, dp, mp, local)
    ids = [dp * SLOT_DEV + n for n in range(SLOT_DEV)]
    for t in range(1, n_dp + 1):
        worker, copy = to_worker(t)
        blocks, _ = blocks_between(blocks_ref, worker, dp, capacity)
        for r in range(capacity):
            part = choose(blocks[r], ids, parts)
            if t < n_dp:
                packed[worker, r] = part
            else:
                landed[dp, r] = part
        if t < n_dp:
            copy.start()
    for t in range(1, n_dp):
        to_worker(t)[1].wait_recv()

    ids, parts = [], []
    for owner in range(n_dp):
        blocks, _ = blocks_between(blocks_ref, dp, owner, capacity)
        ids += blocks
        parts += [landed[owner, r] for r in range(capacity)]
    for slot in range(WORK_DEV):
        sorted_parts[slot] = choose(blocks_ref[dp * WORK_DEV + slot], ids, parts)

    def to_place(t):
        place = (mp + t) % n_mp
        return place, remote(
            spread.at[place], win.at[mp], m_send.at[t], m_recv.at[t], {"mp": place}
        )

    for t in range(1, n_mp + 1):
        place, copy = to_place(t)
        for b, slot in enumerate(pair_slots(place)):
            if t < n_mp:
                spread[place, b] = sorted_parts[slot]
            else:
                win[mp, b] = sorted_parts[slot]
        if t < n_mp:
            copy.start()
    gather.own_piece(0)
    for t in range(1, n_mp):
        to_place(t)[1].wait_recv()
    gather.own_piece(1)
    gather.near_pieces(0)
    gather.far_pieces(0)
    gather.own_piece(2)
    gather.near_pieces(1)
    gather.far_pieces(1)
    gather.near_pieces(2)
    gather.far_pieces(2)
    for i in range(n_mp - 1):
        gather.arrived(i)
    for t in range(1, n_dp):
        to_worker(t)[1].wait_send()
    for t in range(1, n_mp):
        to_place(t)[1].wait_send()
    gather.drain()


def normalize(rows, gain):
    width = rows.shape[1]
    mean = jnp.sum(rows, axis=1, keepdims=True) * (1.0 / width)
    centred = rows - mean
    variance = jnp.sum(centred * centred, axis=1, keepdims=True) * (1.0 / width)
    return centred * lax.rsqrt(variance + norm_eps) * gain


def dot(a, b, contract):
    return lax.dot_general(a, b, ((contract[:1], contract[1:]), ((), ())), preferred_element_type=F32)


def steps_kernel(
    blocks_ref,
    start_ref,
    length_ref,
    win,
    w_input,
    attn_gain,
    w_all,
    final_gain,
    w_mel,
    embed,
    out_ref,
    state,
    residual,
    normed,
    keys,
    values_t,
    heads_t,
    heads,
):
    dp, mp = lax.axis_index("dp"), lax.axis_index("mp")
    groups, width, depth = w_all.shape[0], w_all.shape[3], w_all.shape[2]
    group_heads = width // HEAD_DIM
    half = BLOCK // 2
    tail = HEAD_DIM + 16
    first_row = (mp % 2) * half
    begins, counts = [], []
    for slot in pair_slots(mp):
        block = blocks_ref[dp * WORK_DEV + slot]
        order = block % BLK_UTT
        begins.append(start_ref[block // BLK_UTT] + BLOCK * order - CTX)
        counts.append(jnp.minimum(BLOCK, length_ref[block // BLK_UTT] - BLOCK * order))
    column = lax.broadcasted_iota(jnp.int32, (MEL, BLOCK), 1)
    live = [column < counts[b] for b in range(2)]
    for b in range(2):
        start = jnp.concatenate([win[1, b], win[2, b]], axis=1).astype(F32)
        state[b] = jnp.where(live[b], start, 0.0)
    lane = lax.broadcasted_iota(jnp.int32, (1, width), 1)
    for head in range(group_heads):
        ones = jnp.ones((16, 2 * WIN), BF16)
        values_t[head * tail + HEAD_DIM : (head + 1) * tail, :] = ones
    bias = []
    for b in range(2):
        frame = begins[b] + lax.broadcasted_iota(jnp.int32, (WIN, 1), 0)
        usable = (frame >= 0) & (frame < FRAMES)
        bias.append(jnp.where(usable, 0.0, -1e30).astype(F32))

    totals = None
    for step in range(EULER):
        last = step == EULER - 1
        sizes = (BLOCK, half if last else BLOCK)
        for b in range(2):
            for quarter in range(WIN // LANES):
                merged = win[quarter, b]
                inside = 0 < quarter < WIN // LANES - 1
                if inside:
                    at = slice((quarter - 1) * LANES, quarter * LANES)
                    held = jnp.where(live[b][:, at], 0.0, merged.astype(F32)).astype(BF16)
                    stacked = jnp.concatenate([held, state[b, :, at].astype(BF16)], axis=0)
                    hidden = dot(stacked.T, w_input[...], (1, 0))
                else:
                    hidden = dot(merged.T, w_input[0:MEL, :], (1, 0))
                hidden = hidden + embed[step : step + 1, :]
                row = b * WIN + quarter * LANES
                normed[row : row + LANES, :] = normalize(hidden, attn_gain[...]).astype(BF16)
                if inside:
                    row = b * BLOCK + (quarter - 1) * LANES
                    residual[row : row + LANES, :] = hidden

        def query_rows(b):
            offset = first_row if (last and b) else 0
            return offset, sizes[b]

        def group_body(g, carry):
            key_rows = dot(normed[...], w_all[g, 1], (1, 0)).astype(BF16)
            value_rows = dot(normed[...], w_all[g, 2], (1, 0)).astype(BF16)
            turned = value_rows.T
            for head in range(group_heads):
                values_t[head * tail : head * tail + HEAD_DIM, :] = turned[
                    head * HEAD_DIM : (head + 1) * HEAD_DIM
                ]
            for b in range(2):
                offset, count = query_rows(b)
                at = b * WIN + CTX + offset
                if not isinstance(at, int):
                    at = pl.multiple_of(at, LANES)
                rows = normed[pl.ds(at, count), :]
                scale = math.log2(math.e) / math.sqrt(HEAD_DIM)
                queries = (dot(rows, w_all[g, 0], (1, 0)) * scale).astype(BF16)
                block_keys = key_rows[b * WIN : (b + 1) * WIN].astype(F32)
                edge = [
                    jnp.where(lane == width - 1, bias[b], block_keys).astype(BF16),
                    jnp.where(lane == 0, bias[b], block_keys).astype(BF16),
                ]
                for head in range(group_heads):
                    upper = head >= group_heads // 2
                    flag_lane = 0 if upper else width - 1
                    mine = (lane // HEAD_DIM) == head
                    flag = jnp.where(lane == flag_lane, 1.0, 0.0).astype(BF16)
                    masked = jnp.where(mine, queries, flag)
                    scores = dot(edge[int(upper)], masked, (1, 1))
                    top = jnp.max(scores, axis=0, keepdims=True)
                    weights = jnp.exp2(scores - top).astype(BF16)
                    product = dot(
                        values_t[head * tail : (head + 1) * tail, b * WIN : (b + 1) * WIN],
                        weights,
                        (1, 0),
                    )
                    norm = product[HEAD_DIM : HEAD_DIM + 1, :]
                    out = product[:HEAD_DIM] * (1.0 / norm)
                    heads_t[
                        head * HEAD_DIM : (head + 1) * HEAD_DIM, b * BLOCK : b * BLOCK + count
                    ] = out.astype(BF16)
            lanes = pl.ds(pl.multiple_of(g * width, width), width)
            used = BLOCK + sizes[1]
            heads[0:used, lanes] = heads_t[:, 0:used].T
            return carry

        lax.fori_loop(0, groups, group_body, 0)

        velocities = []
        for b in range(2):
            offset, count = query_rows(b)
            at = b * BLOCK + offset
            if not isinstance(at, int):
                at = pl.multiple_of(at, LANES)
            columns = []
            for n in range(depth // width):
                lanes = slice(n * width, (n + 1) * width)
                term = residual[pl.ds(at, count), lanes]
                for g in range(groups):
                    term = term + dot(
                        heads[b * BLOCK : b * BLOCK + count, g * width : (g + 1) * width],
                        w_all[g, 3, n * width : (n + 1) * width, :],
                        (1, 0),
                    )
                columns.append(term)
            final = normalize(jnp.concatenate(columns, axis=1), final_gain[...]).astype(BF16)
            velocities.append(dot(w_mel[...], final, (1, 1)))
        if not last:
            velocities = [jnp.where(live[b], velocities[b], 0.0) for b in range(2)]
            for b in range(2):
                state[b] = state[b] + velocities[b] * (1.0 / flow_steps)
            second = jnp.where(mp % 2 == 0, velocities[1][:, :half], velocities[1][:, half:])
            part = [velocities[0], second]
            totals = part if totals is None else [totals[b] + part[b] for b in range(2)]
        else:
            places = column[:, :half] + first_row
            part = [
                jnp.where(live[0], velocities[0], 0.0),
                jnp.where(places < counts[1], velocities[1], 0.0),
            ]
            totals = [totals[b] + part[b] for b in range(2)]
            out_ref[0, :, 0:BLOCK] = totals[0].astype(BF16)
            out_ref[0, :, BLOCK : BLOCK + half] = totals[1].astype(BF16)
            out_ref[1, :, 0:BLOCK] = part[0].astype(BF16)
            out_ref[1, :, BLOCK : BLOCK + half] = part[1].astype(BF16)


def outbound_kernel(
    n_dp,
    n_mp,
    capacity,
    blocks_ref,
    mine_ref,
    filled_ref,
    velocity_ref,
    column,
    packed,
    landed,
    m_send,
    m_recv,
    d_send,
    d_recv,
):
    dp, mp = lax.axis_index("dp"), lax.axis_index("mp")
    half = BLOCK // 2
    enter(n_dp, n_mp, dp, mp)

    def to_place(t):
        return remote(
            mine_ref, column.at[mp], m_send.at[t], m_recv.at[t], {"mp": (mp + t) % n_mp}
        )

    for t in range(1, n_mp):
        to_place(t).start()
    column[mp] = mine_ref[...]
    for t in range(1, n_mp):
        to_place(t).wait_recv()

    def block_of(kind, slot):
        pair, which = slot // 3, slot % 3
        one, other = 2 * pair, 2 * pair + 1
        if which == 0:
            return column[one, kind, :, 0:BLOCK]
        if which == 2:
            return column[other, kind, :, 0:BLOCK]
        return jnp.concatenate(
            [column[m, kind, :, BLOCK : BLOCK + half] for m in (one, other)], axis=1
        )

    parts = [block_of(0, slot) for slot in range(WORK_DEV)]

    def to_owner(t):
        owner = (dp + t) % n_dp
        return owner, remote(
            packed.at[owner], landed.at[dp], d_send.at[t], d_recv.at[t], {"dp": owner}
        )

    for t in range(1, n_dp + 1):
        owner, copy = to_owner(t)
        _, places = blocks_between(blocks_ref, dp, owner, capacity)
        for r in range(capacity):
            part = choose(places[r], range(WORK_DEV), parts)
            if t < n_dp:
                packed[owner, r] = part
            else:
                landed[dp, r] = part
        if t < n_dp:
            copy.start()
    for slot in range(WORK_DEV):
        velocity_ref[slot] = block_of(1, slot).astype(F32)
    for t in range(1, n_dp):
        to_owner(t)[1].wait_recv()
    ids, parts = [], []
    for worker in range(n_dp):
        blocks, _ = blocks_between(blocks_ref, worker, dp, capacity)
        ids += blocks
        parts += [landed[worker, r] for r in range(capacity)]
    for local in range(SLOT_DEV):
        order = local % BLK_UTT
        filled_ref[local // BLK_UTT, :, order * BLOCK : (order + 1) * BLOCK] = choose(
            dp * SLOT_DEV + local, ids, parts
        ).astype(F32)
    for t in range(1, n_mp):
        to_place(t).wait_send()
    for t in range(1, n_dp):
        to_owner(t)[1].wait_send()


def shards(
    n_dp,
    n_mp,
    mel_audio,
    start_noise,
    span_start,
    span_length,
    block_route,
    w_input,
    attn_gain,
    w_qkv,
    w_out,
    final_gain,
    w_mel,
):
    capacity = (SLOT_DEV + n_dp - 1) // n_dp
    depth, width = w_qkv.shape[0], w_qkv.shape[2]
    slot_ids = jnp.arange(n_dp * WORK_DEV, dtype=jnp.int32)
    every_slot = jnp.arange(block_route.shape[0], dtype=jnp.int32)
    matches = block_route[None, :] == slot_ids[:, None]
    blocks = jnp.sum(jnp.where(matches, every_slot[None, :], 0), axis=1)

    smem = pl.BlockSpec(memory_space=pltpu.SMEM)
    vmem = pl.BlockSpec(memory_space=pltpu.VMEM)
    hbm = pl.BlockSpec(memory_space=pl.ANY)
    dma = pltpu.SemaphoreType.DMA
    quarters = WIN // LANES
    w_all, win = pl.pallas_call(
        functools.partial(inbound_kernel, n_dp, n_mp, capacity),
        out_shape=(
            jax.ShapeDtypeStruct((n_mp, 4, depth, width), BF16),
            jax.ShapeDtypeStruct((quarters, 2, MEL, LANES), BF16),
        ),
        in_specs=[smem, smem, smem, vmem, vmem, hbm, hbm],
        out_specs=(vmem, vmem),
        scratch_shapes=[
            pltpu.VMEM((n_dp, capacity, MEL, LANES), BF16),
            pltpu.VMEM((n_dp, capacity, MEL, LANES), BF16),
            pltpu.VMEM((WORK_DEV, MEL, LANES), BF16),
            pltpu.VMEM((n_mp, 2, MEL, LANES), BF16),
            dma((1 + n_mp,)),
            dma((n_dp,)),
            dma((n_dp,)),
            dma((n_mp,)),
            dma((n_mp,)),
            *gather_sems(n_mp),
        ],
        compiler_params=pltpu.CompilerParams(
            collective_id=0, has_side_effects=True, vmem_limit_bytes=VMEM_LIMIT
        ),
        name="inbound",
    )(
        blocks,
        span_start,
        span_length,
        mel_audio,
        start_noise,
        w_qkv.transpose(1, 0, 2),
        w_out,
    )

    group_heads = width // HEAD_DIM
    tail = HEAD_DIM + 16
    mine = pl.pallas_call(
        steps_kernel,
        out_shape=jax.ShapeDtypeStruct((2, MEL, BLOCK + BLOCK // 2), BF16),
        in_specs=[smem, smem, smem, vmem, vmem, vmem, vmem, vmem, vmem, vmem],
        out_specs=vmem,
        scratch_shapes=[
            pltpu.VMEM((2, MEL, BLOCK), F32),
            pltpu.VMEM((2 * BLOCK, depth), F32),
            pltpu.VMEM((2 * WIN, depth), BF16),
            pltpu.VMEM((2 * WIN, width), BF16),
            pltpu.VMEM((group_heads * tail, 2 * WIN), BF16),
            pltpu.VMEM((width, 2 * BLOCK), BF16),
            pltpu.VMEM((2 * BLOCK, depth), BF16),
        ],
        compiler_params=pltpu.CompilerParams(vmem_limit_bytes=VMEM_LIMIT),
        name="steps",
    )(
        blocks,
        span_start,
        span_length,
        win,
        w_input,
        attn_gain.reshape(1, -1),
        w_all,
        final_gain.reshape(1, -1),
        w_mel,
        jnp.asarray(time_table(depth)),
    )

    return pl.pallas_call(
        functools.partial(outbound_kernel, n_dp, n_mp, capacity),
        out_shape=(
            jax.ShapeDtypeStruct((UTT_DEV, MEL, SPAN_MAX), F32),
            jax.ShapeDtypeStruct((WORK_DEV, MEL, BLOCK), F32),
        ),
        in_specs=[smem, vmem],
        out_specs=(vmem, vmem),
        scratch_shapes=[
            pltpu.VMEM((n_mp, 2, MEL, BLOCK + BLOCK // 2), BF16),
            pltpu.VMEM((n_dp, capacity, MEL, BLOCK), BF16),
            pltpu.VMEM((n_dp, capacity, MEL, BLOCK), BF16),
            dma((n_mp,)),
            dma((n_mp,)),
            dma((n_dp,)),
            dma((n_dp,)),
        ],
        compiler_params=pltpu.CompilerParams(
            collective_id=1, has_side_effects=True, vmem_limit_bytes=VMEM_LIMIT
        ),
        name="outbound",
    )(blocks, mine)


def solution(mesh):
    n_dp, n_mp = mesh.shape["dp"], mesh.shape["mp"]
    return jax.shard_map(
        functools.partial(shards, n_dp, n_mp),
        mesh=mesh,
        in_specs=(
            P("dp", None, None),
            P("dp", None, None),
            P(),
            P(),
            P(),
            P(),
            P(),
            P(None, None, "mp"),
            P("mp", None),
            P(),
            P(),
        ),
        out_specs=(P("dp", None, None), P("dp", None, None)),
        check_vma=False,
    )
```

```python
import functools
import math

import jax
import jax.numpy as jnp
import numpy as np
from jax import lax
from jax.experimental import pallas as pl
from jax.experimental.pallas import tpu as pltpu
from jax.sharding import PartitionSpec as P

MEL = 80
HEAD_DIM = 64
BLOCK = 256
CTX = 128
BLK_UTT = 4
UTT_DEV = 4
WORK_DEV = 6
EULER = 2
FRAMES = 2048
WIN = 512
SPAN_MAX = 1024
SLOT_DEV = 16
LANES = 128
PIECES = 8

flow_steps = 32.0
norm_eps = 1e-05
MESH = pl.DeviceIdType.MESH
VMEM_LIMIT = 60 * 1024 * 1024
F32 = jnp.float32
BF16 = jnp.bfloat16


def time_table(width):
    half = width // 2
    freqs = np.exp(-math.log(10000.0) * np.arange(half, dtype=np.float64) / half)
    rows = []
    for step in range(EULER):
        angles = 1000.0 * (step / flow_steps) * freqs
        rows.append(np.concatenate([np.sin(angles), np.cos(angles)]))
    return np.stack(rows).astype(np.float32)


def flip(index, bit):
    return index + bit * (1 - 2 * ((index // bit) % 2))


def pick(index, values):
    out = jnp.int32(values[-1])
    for i in range(len(values) - 1):
        out = jnp.where(index == i, jnp.int32(values[i]), out)
    return out


def shard_order(count):
    return [
        sorted((s for s in range(count) if s != m), key=lambda s: (abs(s - m), s))
        for m in range(count)
    ]


def remote(src, dst, send_sem, recv_sem, device):
    return pltpu.make_async_remote_copy(
        src_ref=src,
        dst_ref=dst,
        send_sem=send_sem,
        recv_sem=recv_sem,
        device_id=device,
        device_id_type=MESH,
    )


def enter(n_dp, n_mp, dp, mp):
    barrier = pltpu.get_barrier_semaphore()
    for t in range(1, n_dp):
        pl.semaphore_signal(
            barrier, inc=1, device_id={"dp": (dp + t) % n_dp}, device_id_type=MESH
        )
    for t in range(1, n_mp):
        pl.semaphore_signal(
            barrier, inc=1, device_id={"mp": (mp + t) % n_mp}, device_id_type=MESH
        )
    pl.semaphore_wait(barrier, n_dp + n_mp - 2)


def blocks_between(blocks_ref, worker, owner, capacity):
    blocks = [jnp.int32(-1)] * capacity
    slots = [jnp.int32(-1)] * capacity
    seen = jnp.int32(0)
    for j in range(WORK_DEV):
        block = blocks_ref[0, worker * WORK_DEV + j]
        mine = (block // SLOT_DEV) == owner
        for r in range(capacity):
            here = mine & (seen == r)
            blocks[r] = jnp.where(here, block, blocks[r])
            slots[r] = jnp.where(here, j, slots[r])
        seen = seen + mine.astype(jnp.int32)
    return blocks, slots


def choose(wanted, ids, parts):
    out = jnp.zeros_like(parts[0])
    for n, part in zip(ids, parts):
        out = jnp.where(wanted == n, part, out)
    return out


def pair_slots(mp):
    return 3 * (mp // 2) + 2 * (mp % 2), 3 * (mp // 2) + 1


class WeightGather:
    def __init__(self, n_mp, dp, mp, w_all, sems):
        self.n_mp, self.dp, self.mp, self.w_all = n_mp, dp, mp, w_all
        (self.zs, self.zf, self.zr, self.xs, self.xr, self.ys, self.yr, self.cs, self.cr) = sems
        self.rows = w_all.shape[2] // PIECES
        self.half = self.rows // 2
        base = dp - dp % PIECES
        part = dp % PIECES
        self.part = part
        self.x_peer = {"dp": base + flip(part, 2)}
        self.y_peer = {"dp": base + flip(part, 4)}
        self.c_peer = {"dp": base + flip(part, 1)}
        self.order = shard_order(n_mp)

    def view(self, shard, part, half):
        start = pl.multiple_of(part * self.rows + half * self.half, self.half)
        return self.w_all.at[shard, :, pl.ds(start, self.half), :]

    def shard(self, i):
        return pick(self.mp, [self.order[m][i] for m in range(self.n_mp)])

    def z_copy(self, shard, half, step, send_sem):
        view = self.view(shard, self.part, half)
        return remote(view, view, send_sem, self.zr.at[shard, half], {"mp": self.mp + step})

    def z_arrival(self, shard, half):
        view = self.view(shard, self.part, half)
        sem = self.zf.at[shard, half]
        return remote(view, view, sem, self.zr.at[shard, half], {"mp": (self.mp + 1) % self.n_mp})

    def send_own(self):
        @pl.when(self.mp + 1 < self.n_mp)
        def _():
            for half in range(2):
                self.z_copy(self.mp, half, 1, self.zs.at[0, half]).start()

        @pl.when(self.mp > 0)
        def _():
            for half in range(2):
                self.z_copy(self.mp, half, -1, self.zs.at[1, half]).start()

    def relay(self, shard, half, act):
        @pl.when((shard < self.mp) & (self.mp + 1 < self.n_mp))
        def _():
            act(self.z_copy(shard, half, 1, self.zf.at[shard, half]))

        @pl.when((shard > self.mp) & (self.mp > 0))
        def _():
            act(self.z_copy(shard, half, -1, self.zf.at[shard, half]))

    def x_copy(self, shard, part, half, kind):
        view = self.view(shard, part, half)
        return remote(
            view, view, self.xs.at[shard, kind], self.xr.at[shard, kind], self.x_peer
        )

    def y_copy(self, shard, part, half, kind):
        view = self.view(shard, part, half)
        return remote(
            view, view, self.ys.at[shard, kind], self.yr.at[shard, kind], self.y_peer
        )

    def c_copy(self, shard, part, half, kind):
        view = self.view(shard, part, half)
        return remote(
            view, view, self.cs.at[shard, kind], self.cr.at[shard, kind], self.c_peer
        )

    def own_piece(self, i):
        shard = self.shard(i)
        for half in range(2):
            self.z_arrival(shard, half).wait_recv()
            self.relay(shard, half, lambda copy: copy.start())
            self.x_copy(shard, self.part, half, half).start()
            self.y_copy(shard, self.part, half, half).start()
            self.c_copy(shard, self.part, half, half).start()

    def near_pieces(self, i):
        shard = self.shard(i)
        from_x, from_y = flip(self.part, 2), flip(self.part, 4)
        self.x_copy(shard, from_x, 0, 0).wait_recv()
        self.y_copy(shard, from_x, 0, 2).start()
        self.c_copy(shard, from_x, 0, 2).start()
        self.y_copy(shard, from_y, 0, 0).wait_recv()
        self.c_copy(shard, from_y, 0, 4).start()
        self.y_copy(shard, from_y, 1, 1).wait_recv()
        self.x_copy(shard, from_y, 1, 2).start()
        self.c_copy(shard, from_y, 1, 5).start()
        self.x_copy(shard, from_x, 1, 1).wait_recv()
        self.c_copy(shard, from_x, 1, 3).start()

    def far_pieces(self, i):
        shard = self.shard(i)
        far = flip(flip(self.part, 2), 4)
        self.y_copy(shard, far, 0, 2).wait_recv()
        self.c_copy(shard, far, 0, 6).start()
        self.x_copy(shard, far, 1, 2).wait_recv()
        self.c_copy(shard, far, 1, 7).start()

    def arrived(self, i):
        shard = self.shard(i)
        other = flip(self.part, 1)
        parts = [other, flip(other, 2), flip(other, 4), flip(flip(other, 2), 4)]
        for n, part in enumerate(parts):
            for half in range(2):
                self.c_copy(shard, part, half, 2 * n + half).wait_recv()

    def drain(self):
        for half in range(2):

            @pl.when(self.mp + 1 < self.n_mp)
            def _():
                self.z_copy(self.mp, half, 1, self.zs.at[0, half]).wait_send()

            @pl.when(self.mp > 0)
            def _():
                self.z_copy(self.mp, half, -1, self.zs.at[1, half]).wait_send()

        for i in range(self.n_mp - 1):
            shard = self.shard(i)
            for half in range(2):
                self.relay(shard, half, lambda copy: copy.wait_send())
            for kind in range(3):
                self.x_copy(shard, self.part, 0, kind).wait_send()
                self.y_copy(shard, self.part, 0, kind).wait_send()
            for kind in range(8):
                self.c_copy(shard, self.part, 0, kind).wait_send()


def gather_sems(n_mp):
    dma = pltpu.SemaphoreType.DMA
    return [
        dma((2, 2)),
        dma((n_mp, 2)),
        dma((n_mp, 2)),
        dma((n_mp, 3)),
        dma((n_mp, 3)),
        dma((n_mp, 3)),
        dma((n_mp, 3)),
        dma((n_mp, 8)),
        dma((n_mp, 8)),
    ]


def pack_windows(mel_ref, noise_ref, start_ref, length_ref, dp, mp, local):
    start = start_ref[dp * UTT_DEV + local]
    length = length_ref[dp * UTT_DEV + local]
    first = start - CTX + LANES * mp
    chunk = (first + LANES) // LANES
    offset = first + LANES - chunk * LANES
    count = 2 * BLK_UTT
    zero = jnp.zeros((MEL, LANES), BF16)
    chunks = [zero]
    for n in range(FRAMES // LANES):
        chunks.append(mel_ref[local, :, n * LANES : (n + 1) * LANES])
    bit = 1
    while 2 * bit <= len(chunks):
        bit *= 2
    while bit:
        moved = (chunk // bit) % 2 == 1
        keep = min(len(chunks), count + bit - 1)
        padded = chunks + [zero] * (keep + bit - len(chunks))
        chunks = [jnp.where(moved, padded[n + bit], padded[n]) for n in range(keep)]
        bit //= 2
    row = lax.broadcasted_iota(jnp.int32, (2 * LANES, LANES), 0)
    to = lax.broadcasted_iota(jnp.int32, (2 * LANES, LANES), 1)
    shift = jnp.where(row == to + offset, 1.0, 0.0).astype(BF16)
    both = jnp.concatenate(
        [jnp.concatenate(chunks[2 * k : 2 * k + 2], axis=1) for k in range(BLK_UTT)], axis=0
    )
    shifted = lax.dot_general(
        both, shift, (((1,), (0,)), ((), ())), preferred_element_type=F32
    )
    lane = lax.broadcasted_iota(jnp.int32, (MEL, LANES), 1)
    parts = []
    for k in range(BLK_UTT):
        frame = first + BLOCK * k + lane
        context = (frame >= 0) & (frame < FRAMES) & ((frame < start) | (frame >= start + length))
        own = jnp.minimum(BLOCK, length - BLOCK * k)
        place = LANES * (mp - 1) + lane
        state = (place >= 0) & (place < own)
        noise = jnp.where(
            mp == 2,
            noise_ref[local, :, BLOCK * k + LANES : BLOCK * k + 2 * LANES].astype(F32),
            noise_ref[local, :, BLOCK * k : BLOCK * k + LANES].astype(F32),
        )
        held = jnp.where(context, shifted[k * MEL : (k + 1) * MEL], 0.0)
        parts.append(jnp.where(state, noise, held).astype(BF16))
    return parts


def normalize(rows, gain):
    width = rows.shape[1]
    mean = jnp.sum(rows, axis=1, keepdims=True) * (1.0 / width)
    centred = rows - mean
    variance = jnp.sum(centred * centred, axis=1, keepdims=True) * (1.0 / width)
    return centred * lax.rsqrt(variance + norm_eps) * gain


def dot(a, b, contract):
    return lax.dot_general(a, b, ((contract[:1], contract[1:]), ((), ())), preferred_element_type=F32)


class Steps:
    def __init__(self, plan_ref, dp, mp, win, w_all, weights, scratch):
        self.mp, self.win, self.w_all = mp, win, w_all
        self.w_input, self.attn_gain, self.final_gain, self.w_mel, self.embed = weights
        self.state, self.residual, self.normed, self.values_t, self.heads_t, self.heads = scratch
        self.groups, self.depth, self.width = w_all.shape[0], w_all.shape[2], w_all.shape[3]
        self.group_heads = self.width // HEAD_DIM
        self.half = BLOCK // 2
        self.first_row = (mp % 2) * self.half
        begins, counts = [], []
        for slot in pair_slots(mp):
            at = dp * WORK_DEV + slot
            order = plan_ref[0, at] % BLK_UTT
            begins.append(plan_ref[1, at] + BLOCK * order - CTX)
            counts.append(jnp.minimum(BLOCK, plan_ref[2, at] - BLOCK * order))
        self.counts = counts
        column = lax.broadcasted_iota(jnp.int32, (MEL, BLOCK), 1)
        self.column = column
        self.live = [column < counts[b] for b in range(2)]
        self.lane = lax.broadcasted_iota(jnp.int32, (1, self.width), 1)
        self.bias = []
        for b in range(2):
            frame = begins[b] + lax.broadcasted_iota(jnp.int32, (WIN, 1), 0)
            usable = (frame >= 0) & (frame < FRAMES)
            self.bias.append(jnp.where(usable, 0.0, -1e30).astype(F32))

    def begin(self):
        for b in range(2):
            start = jnp.concatenate([self.win[1, b], self.win[2, b]], axis=1).astype(F32)
            self.state[b] = jnp.where(self.live[b], start, 0.0)
        self.values_t[self.width : self.width + 16, :] = jnp.ones((16, 2 * WIN), BF16)

    def hidden(self, step, b):
        for quarter in range(WIN // LANES):
            merged = self.win[quarter, b]
            inside = 0 < quarter < WIN // LANES - 1
            if inside:
                at = slice((quarter - 1) * LANES, quarter * LANES)
                held = jnp.where(self.live[b][:, at], 0.0, merged.astype(F32)).astype(BF16)
                stacked = jnp.concatenate([held, self.state[b, :, at].astype(BF16)], axis=0)
                hidden = dot(stacked.T, self.w_input[...], (1, 0))
            else:
                hidden = dot(merged.T, self.w_input[0:MEL, :], (1, 0))
            hidden = hidden + self.embed[step : step + 1, :]
            row = b * WIN + quarter * LANES
            self.normed[row : row + LANES, :] = normalize(hidden, self.attn_gain[...]).astype(BF16)
            if inside:
                row = b * BLOCK + (quarter - 1) * LANES
                self.residual[row : row + LANES, :] = hidden

    def rows_of(self, last, b):
        if last and b:
            return self.first_row, self.half
        return 0, BLOCK

    def project(self, g):
        keys = dot(self.normed[...], self.w_all[g, 1], (1, 0)).astype(BF16)
        values = dot(self.normed[...], self.w_all[g, 2], (1, 0)).astype(BF16)
        self.values_t[0 : self.width, :] = values.T
        return keys

    def attend(self, last, g, b, keys):
        offset, count = self.rows_of(last, b)
        at = b * WIN + CTX + offset
        if not isinstance(at, int):
            at = pl.multiple_of(at, LANES)
        scale = math.log2(math.e) / math.sqrt(HEAD_DIM)
        queries = (dot(self.normed[pl.ds(at, count), :], self.w_all[g, 0], (1, 0)) * scale).astype(BF16)
        block_keys = keys[b * WIN : (b + 1) * WIN].astype(F32)
        weights = []
        for upper in range(2):
            flag_lane = 0 if upper else self.width - 1
            flagged = jnp.where(self.lane == flag_lane, self.bias[b], block_keys).astype(BF16)
            flag = jnp.where(self.lane == flag_lane, 1.0, 0.0).astype(BF16)
            masked = []
            for head in range(self.group_heads // 2):
                mine = (self.lane // HEAD_DIM) == head + upper * (self.group_heads // 2)
                masked.append(jnp.where(mine, queries, flag))
            scores = dot(flagged, jnp.concatenate(masked, axis=0), (1, 1))
            top = jnp.max(scores, axis=0, keepdims=True)
            weights.append(jnp.exp2(scores - top).astype(BF16))
        weights = jnp.concatenate(weights, axis=1)
        at = slice(b * WIN, (b + 1) * WIN)
        for head in range(self.group_heads):
            rows = slice(head * HEAD_DIM, (head + 1) * HEAD_DIM)
            with_ones = jnp.concatenate(
                [self.values_t[rows, at], self.values_t[self.width : self.width + 16, at]], axis=0
            )
            product = dot(with_ones, weights[:, head * count : (head + 1) * count], (1, 0))
            out = product[:HEAD_DIM] * (1.0 / product[HEAD_DIM : HEAD_DIM + 1])
            self.heads_t[rows, b * BLOCK : b * BLOCK + count] = out.astype(BF16)

    def collect(self, last, g):
        lanes = pl.ds(pl.multiple_of(g * self.width, self.width), self.width)
        used = BLOCK + self.rows_of(last, 1)[1]
        self.heads[0:used, lanes] = self.heads_t[:, 0:used].T

    def velocity(self, last, b):
        offset, count = self.rows_of(last, b)
        at = b * BLOCK + offset
        if not isinstance(at, int):
            at = pl.multiple_of(at, LANES)
        columns = []
        for n in range(self.depth // self.width):
            lanes = slice(n * self.width, (n + 1) * self.width)
            term = self.residual[pl.ds(at, count), lanes]
            for g in range(self.groups):
                term = term + dot(
                    self.heads[b * BLOCK : b * BLOCK + count, g * self.width : (g + 1) * self.width],
                    self.w_all[g, 3, lanes, :],
                    (1, 0),
                )
            columns.append(term)
        final = normalize(jnp.concatenate(columns, axis=1), self.final_gain[...]).astype(BF16)
        result = dot(self.w_mel[...], final, (1, 1))
        return jnp.where(self.column[:, :count] + offset < self.counts[b], result, 0.0)


def whole_kernel(
    n_dp,
    n_mp,
    capacity,
    plan_ref,
    start_ref,
    length_ref,
    mel_ref,
    noise_ref,
    w_qkv_ref,
    w_out_ref,
    w_input,
    attn_gain,
    final_gain,
    w_mel,
    embed,
    filled_ref,
    velocity_ref,
    w_all,
    win,
    packed,
    landed,
    sorted_parts,
    spread,
    state,
    residual,
    normed,
    values_t,
    heads_t,
    heads,
    mine_ref,
    column,
    packed_out,
    landed_out,
    load_sem,
    d_send,
    d_recv,
    m_send,
    m_recv,
    mo_send,
    mo_recv,
    do_send,
    do_recv,
    *w_sems,
):
    dp, mp = lax.axis_index("dp"), lax.axis_index("mp")
    width = w_all.shape[3]
    half = BLOCK // 2
    loads = [pltpu.make_async_copy(w_qkv_ref, w_all.at[mp, 0:3], load_sem.at[0])]
    for n in range(n_mp):
        loads.append(
            pltpu.make_async_copy(
                w_out_ref.at[:, n * width : (n + 1) * width],
                w_all.at[mp, 3, n * width : (n + 1) * width, :],
                load_sem.at[1 + n],
            )
        )
    for load in loads:
        load.start()
    enter(n_dp, n_mp, dp, mp)
    for load in loads:
        load.wait()
    gather = WeightGather(n_mp, dp, mp, w_all, w_sems)
    gather.send_own()
    blocks_ref = plan_ref

    def to_worker(t):
        worker = (dp + t) % n_dp
        return worker, remote(
            packed.at[worker], landed.at[dp], d_send.at[t], d_recv.at[t], {"dp": worker}
        )

    parts = []
    for local in range(UTT_DEV):
        parts += pack_windows(mel_ref, noise_ref, start_ref, length_ref, dp, mp, local)
    ids = [dp * SLOT_DEV + n for n in range(SLOT_DEV)]
    for t in range(1, n_dp + 1):
        worker, copy = to_worker(t)
        blocks, _ = blocks_between(blocks_ref, worker, dp, capacity)
        for r in range(capacity):
            part = choose(blocks[r], ids, parts)
            if t < n_dp:
                packed[worker, r] = part
            else:
                landed[dp, r] = part
        if t < n_dp:
            copy.start()
    gather.own_piece(0)
    for t in range(1, n_dp):
        to_worker(t)[1].wait_recv()

    ids, parts = [], []
    for owner in range(n_dp):
        blocks, _ = blocks_between(blocks_ref, dp, owner, capacity)
        ids += blocks
        parts += [landed[owner, r] for r in range(capacity)]
    for slot in range(WORK_DEV):
        sorted_parts[slot] = choose(blocks_ref[0, dp * WORK_DEV + slot], ids, parts)

    def to_place(t):
        place = (mp + t) % n_mp
        return place, remote(
            spread.at[place], win.at[mp], m_send.at[t], m_recv.at[t], {"mp": place}
        )

    for t in range(1, n_mp + 1):
        place, copy = to_place(t)
        for b, slot in enumerate(pair_slots(place)):
            if t < n_mp:
                spread[place, b] = sorted_parts[slot]
            else:
                win[mp, b] = sorted_parts[slot]
        if t < n_mp:
            copy.start()
    gather.near_pieces(0)
    for t in range(1, n_mp):
        to_place(t)[1].wait_recv()
    steps = Steps(
        plan_ref,
        dp,
        mp,
        win,
        w_all,
        (w_input, attn_gain, final_gain, w_mel, embed),
        (state, residual, normed, values_t, heads_t, heads),
    )
    steps.begin()
    gather.own_piece(1)
    steps.hidden(0, 0)
    gather.far_pieces(0)
    steps.hidden(0, 1)
    gather.near_pieces(1)
    calls = [
        [lambda: gather.own_piece(2), lambda: gather.far_pieces(1), lambda: gather.arrived(0)],
        [lambda: gather.near_pieces(2), lambda: gather.far_pieces(2), lambda: gather.arrived(1)],
        [lambda: None, lambda: None, lambda: gather.arrived(2)],
        [lambda: None, lambda: None, lambda: None],
    ]
    for n in range(n_mp):
        g = gather.shard(n - 1) if n else mp
        keys = steps.project(g)
        calls[n][0]()
        steps.attend(False, g, 0, keys)
        calls[n][1]()
        steps.attend(False, g, 1, keys)
        steps.collect(False, g)
        calls[n][2]()
    totals = []
    for b in range(2):
        moved = steps.velocity(False, b)
        state[b] = state[b] + moved * (1.0 / flow_steps)
        if b:
            moved = jnp.where(mp % 2 == 0, moved[:, :half], moved[:, half:])
        totals.append(moved)

    for step in range(1, EULER):
        for b in range(2):
            steps.hidden(step, b)

        def group_body(g, carry):
            keys = steps.project(g)
            for b in range(2):
                steps.attend(True, g, b, keys)
            steps.collect(True, g)
            return carry

        lax.fori_loop(0, n_mp, group_body, 0)
    for b in range(2):
        moved = steps.velocity(True, b)
        at = slice(0, BLOCK) if b == 0 else slice(BLOCK, BLOCK + half)
        mine_ref[0, :, at] = (totals[b] + moved).astype(BF16)
        mine_ref[1, :, at] = moved.astype(BF16)

    def to_column(t):
        return remote(
            mine_ref, column.at[mp], mo_send.at[t], mo_recv.at[t], {"mp": (mp + t) % n_mp}
        )

    for t in range(1, n_mp):
        to_column(t).start()
    column[mp] = mine_ref[...]
    for t in range(1, n_mp):
        to_column(t).wait_recv()

    def block_of(kind, slot):
        pair, which = slot // 3, slot % 3
        one, other = 2 * pair, 2 * pair + 1
        if which == 0:
            return column[one, kind, :, 0:BLOCK]
        if which == 2:
            return column[other, kind, :, 0:BLOCK]
        return jnp.concatenate(
            [column[m, kind, :, BLOCK : BLOCK + half] for m in (one, other)], axis=1
        )

    parts = [block_of(0, slot) for slot in range(WORK_DEV)]

    def to_home(t):
        owner = (dp + t) % n_dp
        return owner, remote(
            packed_out.at[owner], landed_out.at[dp], do_send.at[t], do_recv.at[t], {"dp": owner}
        )

    for t in range(1, n_dp + 1):
        owner, copy = to_home(t)
        _, places = blocks_between(blocks_ref, dp, owner, capacity)
        for r in range(capacity):
            part = choose(places[r], range(WORK_DEV), parts)
            if t < n_dp:
                packed_out[owner, r] = part
            else:
                landed_out[dp, r] = part
        if t < n_dp:
            copy.start()
    for slot in range(WORK_DEV):
        velocity_ref[slot] = block_of(1, slot)
    for t in range(1, n_dp):
        to_home(t)[1].wait_recv()
    ids, parts = [], []
    for worker in range(n_dp):
        blocks, _ = blocks_between(blocks_ref, worker, dp, capacity)
        ids += blocks
        parts += [landed_out[worker, r] for r in range(capacity)]
    for local in range(SLOT_DEV):
        order = local % BLK_UTT
        filled_ref[local // BLK_UTT, :, order * BLOCK : (order + 1) * BLOCK] = choose(
            dp * SLOT_DEV + local, ids, parts
        )
    for t in range(1, n_mp):
        to_column(t).wait_send()
    for t in range(1, n_dp):
        to_home(t)[1].wait_send()
    for t in range(1, n_dp):
        to_worker(t)[1].wait_send()
    for t in range(1, n_mp):
        to_place(t)[1].wait_send()
    gather.drain()


def shards(
    n_dp,
    n_mp,
    mel_audio,
    start_noise,
    span_start,
    span_length,
    block_route,
    w_input,
    attn_gain,
    w_qkv,
    w_out,
    final_gain,
    w_mel,
):
    capacity = (SLOT_DEV + n_dp - 1) // n_dp
    depth, width = w_qkv.shape[0], w_qkv.shape[2]
    slot_ids = jnp.arange(n_dp * WORK_DEV, dtype=jnp.int32)
    every_slot = jnp.arange(block_route.shape[0], dtype=jnp.int32)
    matches = block_route[None, :] == slot_ids[:, None]
    facts = jnp.stack(
        [every_slot, jnp.repeat(span_start, BLK_UTT), jnp.repeat(span_length, BLK_UTT)]
    )
    plan = jnp.sum(jnp.where(matches[None], facts[:, None, :], 0), axis=2)

    smem = pl.BlockSpec(memory_space=pltpu.SMEM)
    vmem = pl.BlockSpec(memory_space=pltpu.VMEM)
    hbm = pl.BlockSpec(memory_space=pl.ANY)
    dma = pltpu.SemaphoreType.DMA
    quarters = WIN // LANES
    filled, velocity = pl.pallas_call(
        functools.partial(whole_kernel, n_dp, n_mp, capacity),
        out_shape=(
            jax.ShapeDtypeStruct((UTT_DEV, MEL, SPAN_MAX), BF16),
            jax.ShapeDtypeStruct((WORK_DEV, MEL, BLOCK), BF16),
        ),
        in_specs=[smem, smem, smem, vmem, vmem, hbm, hbm, vmem, vmem, vmem, vmem, vmem],
        out_specs=(vmem, vmem),
        scratch_shapes=[
            pltpu.VMEM((n_mp, 4, depth, width), BF16),
            pltpu.VMEM((quarters, 2, MEL, LANES), BF16),
            pltpu.VMEM((n_dp, capacity, MEL, LANES), BF16),
            pltpu.VMEM((n_dp, capacity, MEL, LANES), BF16),
            pltpu.VMEM((WORK_DEV, MEL, LANES), BF16),
            pltpu.VMEM((n_mp, 2, MEL, LANES), BF16),
            pltpu.VMEM((2, MEL, BLOCK), F32),
            pltpu.VMEM((2 * BLOCK, depth), F32),
            pltpu.VMEM((2 * WIN, depth), BF16),
            pltpu.VMEM((width + 16, 2 * WIN), BF16),
            pltpu.VMEM((width, 2 * BLOCK), BF16),
            pltpu.VMEM((2 * BLOCK, depth), BF16),
            pltpu.VMEM((2, MEL, BLOCK + BLOCK // 2), BF16),
            pltpu.VMEM((n_mp, 2, MEL, BLOCK + BLOCK // 2), BF16),
            pltpu.VMEM((n_dp, capacity, MEL, BLOCK), BF16),
            pltpu.VMEM((n_dp, capacity, MEL, BLOCK), BF16),
            dma((1 + n_mp,)),
            dma((n_dp,)),
            dma((n_dp,)),
            dma((n_mp,)),
            dma((n_mp,)),
            dma((n_mp,)),
            dma((n_mp,)),
            dma((n_dp,)),
            dma((n_dp,)),
            *gather_sems(n_mp),
        ],
        compiler_params=pltpu.CompilerParams(
            collective_id=0, has_side_effects=True, vmem_limit_bytes=VMEM_LIMIT
        ),
        name="whole",
    )(
        plan,
        span_start,
        span_length,
        mel_audio,
        start_noise,
        w_qkv.transpose(1, 0, 2),
        w_out,
        w_input,
        attn_gain.reshape(1, -1),
        final_gain.reshape(1, -1),
        w_mel,
        jnp.asarray(time_table(depth)),
    )
    return filled.astype(F32), velocity.astype(F32)


def solution(mesh):
    n_dp, n_mp = mesh.shape["dp"], mesh.shape["mp"]
    return jax.shard_map(
        functools.partial(shards, n_dp, n_mp),
        mesh=mesh,
        in_specs=(
            P("dp", None, None),
            P("dp", None, None),
            P(),
            P(),
            P(),
            P(),
            P(),
            P(None, None, "mp"),
            P("mp", None),
            P(),
            P(),
        ),
        out_specs=(P("dp", None, None), P("dp", None, None)),
        check_vma=False,
    )
```
